32 devices in a mesh: tau: 4 (over x, core), tile: 8 (over z, y).
Axes of the slice: x: 2, y: 2, z: 4, core: 2. Of those that a mesh axis runs over, the one named last changes fastest.
Arguments:
- occupied: bfloat16 [4, 1024, 128, 128], P('tau', 'tile'), may hold values from -6 to 6
- virtual: bfloat16 [4, 1024, 128, 128], P('tau', 'tile'), may hold values from -0.125 to 0.125
- cos_weights: float32 [4, 4], replicated, may hold values from -1 to 1
- pair_occ: int32 [1536, 16], P('tile'), may hold values from 0 to 127
- pair_virt: int32 [1536, 16], P('tile'), may hold values from 0 to 127
- partial_target_tile: int32 [1536], P('tile'), may hold values from 0 to 255, as said below
Outputs:
- spectrum: float32 [4, 256, 128, 128], P(None, 'tile', 'tau')
The draws below stay inside these ranges and needn't reach their ends.
Inputs may be any that keep to these rules, and one draw needn't show every extreme that they name: `partial_target_tile`: within each aligned block of 192 entries, no owner (values d * 32 to (d + 1) * 32 - 1 for owner d) is named more than 48 times; one owner is named exactly 48 times in every block.
All inputs are finite; a program needn't handle non-finite values.
Results may differ from the reference program's by a relative error of at most 0.0003.
Values sent between devices are 32-bit elements; how exact they have to be, the bound alone decides.
A program may use at most 192 MiB of HBM per device.

```python
import math
import jax
import jax.numpy as jnp
from jax import lax

TILE = 128
TERMS = 16
NFREQ = 4
SLOT_DEV = 128
PART_DEV = 192
CHI_DEV = 32
NTAU = 4
NOCC = 1024
NPART = 1536
NCHI = 256
CAP = 48


def draw_partial_target_tile(key, part):
    owners = NPART // PART_DEV
    first, second, third, fourth = jax.random.split(jax.random.fold_in(key, 7), 4)
    complete_holder = jax.random.randint(first, (), 0, owners)
    owner_preference = jax.random.randint(second, (owners, owners), 0, 1 << 19)
    random_perturbation = jax.random.randint(third, (owners, owners, CAP), 0, 1 << 19)
    holder_indices = jnp.arange(owners, dtype=jnp.int32)
    extra_credit = jnp.where(holder_indices == complete_holder, 1 << 20, 0).astype(jnp.int32)
    ranking_value = owner_preference[:, :, None] + random_perturbation + extra_credit[None, :, None]
    places = jnp.arange(owners * CAP, dtype=jnp.int32).reshape(owners, CAP)
    ranking_value = ranking_value * (owners * CAP) + places[None]
    flat = ranking_value.reshape(owners, owners * CAP)
    _, chosen = lax.top_k(flat, PART_DEV)
    owner = (chosen // CAP).astype(jnp.int32)
    within = jax.random.randint(fourth, (owners, PART_DEV), 0, CHI_DEV)
    return (owner * CHI_DEV + within).reshape(-1).astype(jnp.int32)


def touch_ends(drawn, stream_key, low, largest):
    longest = drawn.shape.index(max(drawn.shape))
    spots = []
    for shift in (0, 1):
        where = [jax.random.randint(jax.random.fold_in(stream_key, axis), (), 0, length) for axis, length in enumerate(drawn.shape)]
        where[longest] = (where[longest] + shift) % drawn.shape[longest]
        spots.append(tuple(where))
    return drawn.at[spots[0]].set(low).at[spots[1]].set(largest)


def level_of(rng, dims, pieces, least, largest):
    factor_of = 1.0
    for position, parts in pieces:
        draws = jax.random.uniform(jax.random.fold_in(jax.random.fold_in(rng, 6), position), (parts,), jnp.float32, least / len(pieces), largest / len(pieces))
        factor_of = factor_of * jnp.repeat(jnp.exp(draws), dims[position] // parts).reshape((-1,) + (1,) * (len(dims) - 1 - position))
    return factor_of


def noise(rng, dims, width, reach, cuts=(), held_as=jnp.bfloat16):
    array = width * jax.random.normal(rng, dims, jnp.float32)
    if cuts:
        array = array * level_of(rng, dims, cuts, -0.22, 0.18)
    return jnp.clip(array, -reach, reach).astype(held_as)


def setup_inputs(seed: int = 0) -> dict:
    splits = jax.random.split(jax.random.key(seed), 7)
    return {
        "occupied": noise(splits[0], (NTAU, NOCC, TILE, TILE), 1.0, 6.0, ((0, 4), (1, 8))),
        "virtual": noise(splits[1], (NTAU, NOCC, TILE, TILE), (TILE * TERMS) ** -0.5, 0.125, ((0, 4), (1, 8))),
        "cos_weights": jnp.clip(jax.random.uniform(splits[2], (NFREQ, NTAU), jnp.float32, -1.0, 1.0), -1.0, 1.0),
        "pair_occ": touch_ends(jax.random.randint(splits[3], (NPART, TERMS), 0, SLOT_DEV), jax.random.fold_in(splits[3], 1), 0, SLOT_DEV - 1).astype(jnp.int32),
        "pair_virt": touch_ends(jax.random.randint(splits[4], (NPART, TERMS), 0, SLOT_DEV), jax.random.fold_in(splits[4], 1), 0, SLOT_DEV - 1).astype(jnp.int32),
        "partial_target_tile": draw_partial_target_tile(jax.random.fold_in(splits[6], 71), 0),
    }


def reference(occupied, virtual, cos_weights, pair_occ, pair_virt, partial_target_tile):
    owner_base = (jnp.arange(NPART, dtype=jnp.int32) // PART_DEV) * SLOT_DEV
    occ_global = (pair_occ + owner_base[:, None]).astype(jnp.int32)
    virt_global = (pair_virt + owner_base[:, None]).astype(jnp.int32)
    group = math.gcd(NPART, 16)
    count = NPART // group
    occ_blocks = occ_global.reshape(count, group, TERMS)
    virt_blocks = virt_global.reshape(count, group, TERMS)
    dest_blocks = partial_target_tile.astype(jnp.int32).reshape(count, group)

    def time_step(spectrum, step_index):
        occ_now = lax.dynamic_index_in_dim(occupied, step_index, 0, keepdims=False)
        virt_now = lax.dynamic_index_in_dim(virtual, step_index, 0, keepdims=False)

        def add_block(chi_time, items):
            left = jnp.take(occ_now, items[0], axis=0).astype(jnp.float32)
            right = jnp.take(virt_now, items[1], axis=0).astype(jnp.float32)
            product = jnp.einsum("bjrk,bjkc->brc", left, right, precision=lax.Precision.HIGHEST)
            return chi_time.at[items[2]].add(product), None

        chi_time, _ = lax.scan(add_block, jnp.zeros((NCHI, TILE, TILE), jnp.float32),
                               (occ_blocks, virt_blocks, dest_blocks))
        weights = lax.dynamic_index_in_dim(cos_weights, step_index, 1, keepdims=False)
        return spectrum + weights[:, None, None, None] * chi_time[None], None

    spectrum, _ = lax.scan(time_step, jnp.zeros((NFREQ, NCHI, TILE, TILE), jnp.float32),
                           jnp.arange(NTAU, dtype=jnp.int32))
    return spectrum
```

```python
import functools

import jax
import jax.numpy as jnp
from jax import lax
from jax.experimental import pallas as pl
from jax.experimental.pallas import tpu as pltpu
from jax.sharding import PartitionSpec as P

CHI_DEV = 32
CHUNKS = 4


def products_kernel(first, terms, chi_dev, occ_idx, virt_idx, target, occ, virt, out):
    owners, groups, span, rows, width = out.shape
    count = target.shape[0]

    @pl.loop(0, owners)
    def _(d):
        out[d] = jnp.zeros(out.shape[1:], out.dtype)

    @pl.loop(0, count)
    def _(p):
        tile = target[p]
        owner = tile // chi_dev
        place = tile - owner * chi_dev - first

        @pl.when((place >= 0) & (place < span))
        def _():
            acc = None
            step = 2 if terms % 2 == 0 else 1
            for j in range(0, terms, step):
                base = p * terms + j
                left = [occ[occ_idx[base + i]] for i in range(step)]
                right = [virt[virt_idx[base + i]] for i in range(step)]
                dot = jnp.dot(
                    jnp.concatenate(left, axis=1),
                    jnp.concatenate(right, axis=0),
                    preferred_element_type=jnp.float32,
                )
                acc = dot if acc is None else acc + dot
            for g in range(groups):
                out[owner, g, place] += acc[g * rows : (g + 1) * rows]


def products(occ, virt, occ_idx, virt_idx, target, first, span, owners, groups):
    terms = occ_idx.shape[1]
    size = occ.shape[1]
    smem = pl.BlockSpec(memory_space=pltpu.SMEM)
    vmem = pl.BlockSpec(memory_space=pltpu.VMEM)
    return pl.pallas_call(
        functools.partial(products_kernel, first, terms, CHI_DEV),
        out_shape=jax.ShapeDtypeStruct((owners, groups, span, size // groups, size), jnp.float32),
        in_specs=[smem, smem, smem, vmem, vmem],
        out_specs=vmem,
        compiler_params=pltpu.CompilerParams(vmem_limit_bytes=56 * 1024 * 1024),
        cost_estimate=pl.CostEstimate(
            flops=2 * target.shape[0] * terms * size**3 * span // CHI_DEV,
            bytes_accessed=occ.size * 4 + owners * span * size * size * 4,
            transcendentals=0,
        ),
    )(occ_idx.reshape(-1), virt_idx.reshape(-1), target, occ, virt)


def body(occupied, virtual, cos_weights, pair_occ, pair_virt, partial_target_tile):
    owners = lax.axis_size("tile")
    groups = lax.axis_size("tau")
    span = CHI_DEV // CHUNKS
    results = []
    for q in range(CHUNKS):
        local = products(
            occupied[0], virtual[0], pair_occ, pair_virt, partial_target_tile,
            q * span, span, owners, groups,
        )
        flat = local.reshape((owners * groups * span,) + local.shape[3:])
        owned = lax.psum_scatter(flat, "tile", scatter_dimension=0, tiled=True)
        swapped = lax.all_to_all(owned, "tau", split_axis=0, concat_axis=0, tiled=True)
        by_time = swapped.reshape((groups, span) + local.shape[3:])
        part = sum(cos_weights[:, t, None, None, None] * by_time[t][None] for t in range(groups))
        results.append(part)
    return jnp.concatenate(results, axis=1)


def solution(mesh):
    in_specs = (
        P("tau", "tile", None, None),
        P("tau", "tile", None, None),
        P(),
        P("tile", None),
        P("tile", None),
        P("tile"),
    )
    out_specs = P(None, "tile", "tau", None)
    return jax.shard_map(body, mesh=mesh, in_specs=in_specs, out_specs=out_specs, check_vma=False)
```

```python
import functools

import jax
import jax.numpy as jnp
from jax import lax
from jax.experimental import pallas as pl
from jax.experimental.pallas import tpu as pltpu
from jax.sharding import PartitionSpec as P

CHI_DEV = 32
UNIT = 4
BUDGET = 46 * 1024 * 1024
MESH = pl.DeviceIdType.MESH


def products_kernel(first, terms, chi_dev, occ_idx, virt_idx, target, occ, virt, out):
    owners, units, groups, each, rows, width = out.shape
    span = units * each
    count = target.shape[0]

    @pl.loop(0, owners)
    def _(d):
        out[d] = jnp.zeros(out.shape[1:], out.dtype)

    @pl.loop(0, count)
    def _(p):
        tile = target[p]
        owner = tile // chi_dev
        place = tile - owner * chi_dev - first

        @pl.when((place >= 0) & (place < span))
        def _():
            unit = place // each
            acc = None
            step = 2 if terms % 2 == 0 else 1
            for j in range(0, terms, step):
                base = p * terms + j
                left = [occ[occ_idx[base + i]] for i in range(step)]
                right = [virt[virt_idx[base + i]] for i in range(step)]
                dot = jnp.dot(
                    jnp.concatenate(left, axis=1),
                    jnp.concatenate(right, axis=0),
                    preferred_element_type=jnp.float32,
                )
                acc = dot if acc is None else acc + dot
            for g in range(groups):
                out[owner, unit, g, place - unit * each] += acc[g * rows : (g + 1) * rows]


def products(occ, virt, occ_idx, virt_idx, target, first, span, each, owners, groups):
    terms = occ_idx.shape[1]
    size = occ.shape[1]
    smem = pl.BlockSpec(memory_space=pltpu.SMEM)
    vmem = pl.BlockSpec(memory_space=pltpu.VMEM)
    return pl.pallas_call(
        functools.partial(products_kernel, first, terms, CHI_DEV),
        out_shape=jax.ShapeDtypeStruct(
            (owners, span // each, groups, each, size // groups, size), jnp.float32
        ),
        in_specs=[smem, smem, smem, vmem, vmem],
        out_specs=vmem,
        compiler_params=pltpu.CompilerParams(vmem_limit_bytes=56 * 1024 * 1024),
        cost_estimate=pl.CostEstimate(
            flops=2 * target.shape[0] * terms * size**3 * span // CHI_DEV,
            bytes_accessed=occ.size * 4 + owners * span * size * size * 4,
            transcendentals=0,
        ),
    )(occ_idx.reshape(-1), virt_idx.reshape(-1), target, occ, virt)


def line_slots(n):
    if n == 1:
        return 0
    return 1 if n == 2 else 2 * (n - 1)


class Line:
    def __init__(self, n, place, device, own, slots, send_sem, recv_sem, hold=None):
        self.hold = hold
        self.n, self.place, self.device = n, place, device
        self.own, self.slots, self.send_sem, self.recv_sem = own, slots, send_sem, recv_sem

    def slot(self, right, d):
        if right:
            return d - 1
        return d if self.n == 2 else self.n - 1 + d

    def copy(self, right, u, d, src, back=False):
        s = self.slot(right, d)
        k = u * line_slots(self.n) + s
        return pltpu.make_async_remote_copy(
            src_ref=src,
            dst_ref=self.slots.at[s, u],
            send_sem=self.send_sem.at[k],
            recv_sem=self.recv_sem.at[k],
            device_id={"tile": self.device(1 if right != back else -1)},
            device_id_type=MESH,
        )

    def routes(self):
        for right in (True, False):
            for d in range(self.n - 1, 0, -1) if right else range(self.n - 1):
                yield right, d

    def launch(self, u):
        for right, d in self.routes():
            @pl.when(self.place == (0 if right else self.n - 1))
            def _():
                self.copy(right, u, d, self.own(d, u)).start()

    def merge(self, u):
        if self.n == 2:
            return
        for right, d in self.routes():
            inner = (self.place > 0) & (self.place < d) if right else (
                (self.place < self.n - 1) & (self.place > d))

            @pl.when(inner)
            def _():
                here = self.slots.at[self.slot(right, d), u]
                copy = self.copy(right, u, d, here)
                copy.wait_recv()
                own = self.own(d, u)
                if self.hold is not None:
                    buffer, sem = self.hold
                    fetch = pltpu.make_async_copy(own, buffer, sem)
                    fetch.start()
                    fetch.wait()
                    own = buffer
                here[...] += own[...]
                copy.start()

    def final(self, u, into):
        for right in (True, False):
            @pl.when(self.place > 0 if right else self.place < self.n - 1)
            def _():
                k = self.slot(right, self.place)
                here = self.slots.at[k, u]
                self.copy(right, u, self.place, here, back=True).wait_recv()
                into[...] += here[...]

    def drain(self, u):
        for right, d in self.routes():
            @pl.when(self.place < d if right else self.place > d)
            def _():
                self.copy(right, u, d, self.slots.at[self.slot(right, d), u]).wait_send()


def scatter_kernel(ny, nz, groups, weights, dense, out, mine, y_slots, z_slots, times,
                   load_sem, y_send, y_recv, z_send, z_recv, t_send, t_recv, hold, hold_sem):
    tau = lax.axis_index("tau")
    tile = lax.axis_index("tile")
    z, y = tile // ny, tile % ny
    units = mine.shape[0]
    each = mine.shape[3]
    freqs = out.shape[0]

    y_line = Line(ny, y, lambda step: tile + step, lambda d, u: dense.at[:, d, u],
                  y_slots, y_send, y_recv, (hold, hold_sem))
    z_line = Line(nz, z, lambda step: tile + step * ny, lambda d, u: mine.at[u, d],
                  z_slots, z_send, z_recv)

    barrier = pltpu.get_barrier_semaphore()
    for step in range(1, groups):
        pl.semaphore_signal(barrier, inc=1, device_id={"tau": (tau + step) % groups},
                            device_id_type=MESH)
    for step in range(1, ny):
        pl.semaphore_signal(barrier, inc=1, device_id={"tile": z * ny + (y + step) % ny},
                            device_id_type=MESH)
    for step in range(1, nz):
        pl.semaphore_signal(barrier, inc=1, device_id={"tile": (z + step) % nz * ny + y},
                            device_id_type=MESH)
    pl.semaphore_wait(barrier, groups - 1 + ny - 1 + nz - 1)

    def load(u):
        return pltpu.make_async_copy(dense.at[:, y, u], mine.at[u], load_sem.at[u])

    def swap(u, step):
        other = (tau + step) % groups
        return pltpu.make_async_remote_copy(
            src_ref=mine.at[u, z, other],
            dst_ref=times.at[u, tau],
            send_sem=t_send.at[u * groups + step],
            recv_sem=t_recv.at[u * groups + tau],
            device_id={"tau": other},
            device_id_type=MESH,
        )

    def arrived(u, source):
        return pltpu.make_async_remote_copy(
            src_ref=mine.at[u, z, 0],
            dst_ref=times.at[u, source],
            send_sem=t_send.at[u * groups],
            recv_sem=t_recv.at[u * groups + source],
            device_id={"tau": source},
            device_id_type=MESH,
        )

    @pl.loop(0, units)
    def _(u):
        y_line.launch(u)
        load(u).start()

    @pl.loop(0, units + 2)
    def _(t):
        @pl.when(t < units)
        def _():
            load(t).wait()
            y_line.merge(t)
            y_line.final(t, mine.at[t])
            z_line.launch(t)

        @pl.when((t >= 1) & (t < units + 1))
        def _():
            u = t - 1
            z_line.merge(u)
            z_line.final(u, mine.at[u, z])
            for step in range(1, groups):
                swap(u, step).start()
            times[u, tau] = mine[u, z, tau]

        @pl.when(t >= 2)
        def _():
            u = t - 2
            for step in range(1, groups):
                arrived(u, (tau + step) % groups).wait_recv()
            for e in range(each):
                for k in range(freqs):
                    total = weights[k, 0] * times[u, 0, e]
                    for s in range(1, groups):
                        total += weights[k, s] * times[u, s, e]
                    out[k, u * each + e] = total

    @pl.loop(0, units)
    def _(u):
        y_line.drain(u)
        z_line.drain(u)
        for step in range(1, groups):
            swap(u, step).wait_send()


def scatter(dense, weights, ny, nz, groups):
    owners, units, _, each, rows, width = dense.shape
    freqs = weights.shape[0]
    block = (groups, each, rows, width)
    ys, zs = max(line_slots(ny), 1), max(line_slots(nz), 1)
    dma = pltpu.SemaphoreType.DMA
    return pl.pallas_call(
        functools.partial(scatter_kernel, ny, nz, groups),
        out_shape=jax.ShapeDtypeStruct((freqs, units * each, rows, width), jnp.float32),
        in_specs=[pl.BlockSpec(memory_space=pltpu.SMEM), pl.BlockSpec(memory_space=pl.ANY)],
        out_specs=pl.BlockSpec(memory_space=pltpu.VMEM),
        scratch_shapes=[
            pltpu.VMEM((units, nz) + block, jnp.float32),
            pltpu.VMEM((ys, units, nz) + block, jnp.float32),
            pltpu.VMEM((zs, units) + block, jnp.float32),
            pltpu.VMEM((units, groups, each, rows, width), jnp.float32),
            dma((units,)),
            dma((units * ys,)),
            dma((units * ys,)),
            dma((units * zs,)),
            dma((units * zs,)),
            dma((units * groups,)),
            dma((units * groups,)),
            pltpu.VMEM((nz,) + block if ny > 2 else (8, 128), jnp.float32),
            dma,
        ],
        compiler_params=pltpu.CompilerParams(
            collective_id=0, has_side_effects=True, vmem_limit_bytes=58 * 1024 * 1024),
    )(weights, dense.reshape((nz, ny) + dense.shape[1:]))


def body(occupied, virtual, cos_weights, pair_occ, pair_virt, partial_target_tile):
    owners = lax.axis_size("tile")
    groups = lax.axis_size("tau")
    size = occupied.shape[2]
    ny = 1
    while 2 * ny * 2 * ny <= owners:
        ny *= 2
    nz = owners // ny
    tile_bytes = 4 * size * size
    span = CHI_DEV
    while span > UNIT and span * tile_bytes * (
        nz * (1 + line_slots(ny)) + line_slots(nz) + 2
    ) > BUDGET:
        span //= 2
    results = []
    for q in range(CHI_DEV // span):
        dense = products(
            occupied[0], virtual[0], pair_occ, pair_virt, partial_target_tile,
            q * span, span, min(UNIT, span), owners, groups,
        )
        results.append(scatter(dense, cos_weights, ny, nz, groups))
    return results[0] if len(results) == 1 else jnp.concatenate(results, axis=1)


def solution(mesh):
    in_specs = (
        P("tau", "tile", None, None),
        P("tau", "tile", None, None),
        P(),
        P("tile", None),
        P("tile", None),
        P("tile"),
    )
    out_specs = P(None, "tile", "tau", None)
    return jax.shard_map(body, mesh=mesh, in_specs=in_specs, out_specs=out_specs, check_vma=False)
```

```python
import functools
import math

import jax
import jax.numpy as jnp
from jax import lax
from jax.experimental import pallas as pl
from jax.experimental.pallas import tpu as pltpu
from jax.sharding import PartitionSpec as P

CHI_DEV = 32
UNIT = 4
BUDGET = 46 * 1024 * 1024
MESH = pl.DeviceIdType.MESH


def products_kernel(first, terms, chi_dev, occ_idx, virt_idx, target, occ, virt, out):
    owners, units, groups, each, rows, width = out.shape
    span = units * each
    count = target.shape[0]

    @pl.loop(0, owners)
    def _(d):
        out[d] = jnp.zeros(out.shape[1:], out.dtype)

    unroll = math.gcd(count, 4) if span == chi_dev else 1

    @pl.loop(0, count, unroll=unroll)
    def _(p):
        tile = target[p]
        owner = tile // chi_dev
        place = tile - owner * chi_dev - first

        def add():
            unit = place // each
            left = [occ[occ_idx[p * terms + j]] for j in range(terms)]
            right = [virt[virt_idx[p * terms + j]] for j in range(terms)]
            acc = jnp.dot(
                jnp.concatenate(left, axis=1),
                jnp.concatenate(right, axis=0),
                preferred_element_type=jnp.float32,
            )
            for g in range(groups):
                out[owner, unit, g, place - unit * each] += acc[g * rows : (g + 1) * rows]

        if span == chi_dev:
            add()
        else:
            pl.when((place >= 0) & (place < span))(add)


def products(occ, virt, occ_idx, virt_idx, target, first, span, each, owners, groups):
    terms = occ_idx.shape[1]
    size = occ.shape[1]
    smem = pl.BlockSpec(memory_space=pltpu.SMEM)
    vmem = pl.BlockSpec(memory_space=pltpu.VMEM)
    return pl.pallas_call(
        functools.partial(products_kernel, first, terms, CHI_DEV),
        out_shape=jax.ShapeDtypeStruct(
            (owners, span // each, groups, each, size // groups, size), jnp.float32
        ),
        in_specs=[smem, smem, smem, vmem, vmem],
        out_specs=vmem,
        compiler_params=pltpu.CompilerParams(vmem_limit_bytes=56 * 1024 * 1024),
        cost_estimate=pl.CostEstimate(
            flops=2 * target.shape[0] * terms * size**3 * span // CHI_DEV,
            bytes_accessed=occ.size * 4 + owners * span * size * size * 4,
            transcendentals=0,
        ),
    )(occ_idx.reshape(-1), virt_idx.reshape(-1), target, occ, virt)


def line_slots(n):
    if n == 1:
        return 0
    return 1 if n == 2 else 2 * (n - 1)


class Line:
    def __init__(self, n, place, device, own, slots, send_sem, recv_sem, hold=None):
        self.hold = hold
        self.n, self.place, self.device = n, place, device
        self.own, self.slots, self.send_sem, self.recv_sem = own, slots, send_sem, recv_sem

    def slot(self, right, d):
        if right:
            return d - 1
        return d if self.n == 2 else self.n - 1 + d

    def copy(self, right, u, d, src, back=False):
        s = self.slot(right, d)
        k = u * line_slots(self.n) + s
        return pltpu.make_async_remote_copy(
            src_ref=src,
            dst_ref=self.slots.at[s, u],
            send_sem=self.send_sem.at[k],
            recv_sem=self.recv_sem.at[k],
            device_id={"tile": self.device(1 if right != back else -1)},
            device_id_type=MESH,
        )

    def routes(self):
        for right in (True, False):
            for d in range(self.n - 1, 0, -1) if right else range(self.n - 1):
                yield right, d

    def launch(self, u):
        for right, d in self.routes():
            @pl.when(self.place == (0 if right else self.n - 1))
            def _():
                self.copy(right, u, d, self.own(d, u)).start()

    def merge(self, u):
        if self.n == 2:
            return
        for right, d in self.routes():
            inner = (self.place > 0) & (self.place < d) if right else (
                (self.place < self.n - 1) & (self.place > d))

            @pl.when(inner)
            def _():
                here = self.slots.at[self.slot(right, d), u]
                copy = self.copy(right, u, d, here)
                copy.wait_recv()
                own = self.own(d, u)
                if self.hold is not None:
                    buffer, sem = self.hold
                    fetch = pltpu.make_async_copy(own, buffer, sem)
                    fetch.start()
                    fetch.wait()
                    own = buffer
                here[...] += own[...]
                copy.start()

    def final(self, u, into):
        for right in (True, False):
            @pl.when(self.place > 0 if right else self.place < self.n - 1)
            def _():
                k = self.slot(right, self.place)
                here = self.slots.at[k, u]
                self.copy(right, u, self.place, here, back=True).wait_recv()
                into[...] += here[...]

    def drain(self, u):
        for right, d in self.routes():
            @pl.when(self.place < d if right else self.place > d)
            def _():
                self.copy(right, u, d, self.slots.at[self.slot(right, d), u]).wait_send()


def scatter_kernel(ny, nz, groups, weights, dense, out, mine, y_slots, z_slots, times,
                   load_sem, y_send, y_recv, z_send, z_recv, t_send, t_recv, hold, hold_sem,
                   both, z2_slots, y2_slots, both_sem, z2_send, z2_recv, y2_send, y2_recv):
    tau = lax.axis_index("tau")
    tile = lax.axis_index("tile")
    z, y = tile // ny, tile % ny
    units = mine.shape[0]
    last = units - 1
    each = mine.shape[3]
    freqs = out.shape[0]

    y_line = Line(ny, y, lambda step: tile + step, lambda d, u: dense.at[:, d, u],
                  y_slots, y_send, y_recv, (hold, hold_sem))
    z_line = Line(nz, z, lambda step: tile + step * ny, lambda d, u: mine.at[u, d],
                  z_slots, z_send, z_recv)

    z2_line = Line(nz, z, z_line.device, lambda d, u: both.at[d], z2_slots, z2_send, z2_recv)
    y2_line = Line(ny, y, y_line.device, lambda d, u: both.at[z, d], y2_slots, y2_send, y2_recv)

    barrier = pltpu.get_barrier_semaphore()
    for step in range(1, groups):
        pl.semaphore_signal(barrier, inc=1, device_id={"tau": (tau + step) % groups},
                            device_id_type=MESH)
    for step in range(1, ny):
        pl.semaphore_signal(barrier, inc=1, device_id={"tile": z * ny + (y + step) % ny},
                            device_id_type=MESH)
    for step in range(1, nz):
        pl.semaphore_signal(barrier, inc=1, device_id={"tile": (z + step) % nz * ny + y},
                            device_id_type=MESH)
    pl.semaphore_wait(barrier, groups - 1 + ny - 1 + nz - 1)

    def load(u):
        return pltpu.make_async_copy(dense.at[:, y, u], mine.at[u], load_sem.at[u])

    def swap(u, step):
        other = (tau + step) % groups
        return pltpu.make_async_remote_copy(
            src_ref=mine.at[u, z, other],
            dst_ref=times.at[u, tau],
            send_sem=t_send.at[u * groups + step],
            recv_sem=t_recv.at[u * groups + tau],
            device_id={"tau": other},
            device_id_type=MESH,
        )

    def arrived(u, source):
        return pltpu.make_async_remote_copy(
            src_ref=mine.at[u, z, 0],
            dst_ref=times.at[u, source],
            send_sem=t_send.at[u * groups],
            recv_sem=t_recv.at[u * groups + source],
            device_id={"tau": source},
            device_id_type=MESH,
        )

    whole = pltpu.make_async_copy(dense.at[:, :, last], both, both_sem)
    whole.start()

    @pl.loop(0, last)
    def _(u):
        y_line.launch(u)
        load(u).start()

    whole.wait()
    z2_line.launch(0)
    z2_line.merge(0)

    @pl.loop(0, units + 2)
    def _(t):
        @pl.when(t < last)
        def _():
            load(t).wait()
            y_line.merge(t)
            y_line.final(t, mine.at[t])
            z_line.launch(t)

        @pl.when(t == 0)
        def _():
            z2_line.final(0, both.at[z])
            y2_line.launch(0)

        @pl.when((t >= 1) & (t < units))
        def _():
            u = t - 1
            z_line.merge(u)
            z_line.final(u, mine.at[u, z])

        @pl.when(t == units)
        def _():
            y2_line.merge(0)
            mine[last, z] = both[z, y]
            y2_line.final(0, mine.at[last, z])

        @pl.when((t >= 1) & (t < units + 1))
        def _():
            u = t - 1
            for step in range(1, groups):
                swap(u, step).start()
            times[u, tau] = mine[u, z, tau]

        @pl.when(t >= 2)
        def _():
            u = t - 2
            for step in range(1, groups):
                arrived(u, (tau + step) % groups).wait_recv()
            for e in range(each):
                for k in range(freqs):
                    total = weights[k, 0] * times[u, 0, e]
                    for s in range(1, groups):
                        total += weights[k, s] * times[u, s, e]
                    out[k, u * each + e] = total

    z2_line.drain(0)
    y2_line.drain(0)

    @pl.loop(0, last)
    def _(u):
        y_line.drain(u)
        z_line.drain(u)

    @pl.loop(0, units)
    def _(u):
        for step in range(1, groups):
            swap(u, step).wait_send()


def scatter(dense, weights, ny, nz, groups):
    owners, units, _, each, rows, width = dense.shape
    freqs = weights.shape[0]
    block = (groups, each, rows, width)
    ys, zs = max(line_slots(ny), 1), max(line_slots(nz), 1)
    dma = pltpu.SemaphoreType.DMA
    return pl.pallas_call(
        functools.partial(scatter_kernel, ny, nz, groups),
        out_shape=jax.ShapeDtypeStruct((freqs, units * each, rows, width), jnp.float32),
        in_specs=[pl.BlockSpec(memory_space=pltpu.SMEM), pl.BlockSpec(memory_space=pl.ANY)],
        out_specs=pl.BlockSpec(memory_space=pltpu.VMEM),
        scratch_shapes=[
            pltpu.VMEM((units, nz) + block, jnp.float32),
            pltpu.VMEM((ys, units, nz) + block, jnp.float32),
            pltpu.VMEM((zs, units) + block, jnp.float32),
            pltpu.VMEM((units, groups, each, rows, width), jnp.float32),
            dma((units,)),
            dma((units * ys,)),
            dma((units * ys,)),
            dma((units * zs,)),
            dma((units * zs,)),
            dma((units * groups,)),
            dma((units * groups,)),
            pltpu.VMEM((nz,) + block if ny > 2 else (8, 128), jnp.float32),
            dma,
            pltpu.VMEM((nz, ny) + block, jnp.float32),
            pltpu.VMEM((zs, 1, ny) + block, jnp.float32),
            pltpu.VMEM((ys, 1) + block, jnp.float32),
            dma,
            dma((zs,)),
            dma((zs,)),
            dma((ys,)),
            dma((ys,)),
        ],
        compiler_params=pltpu.CompilerParams(
            collective_id=0, has_side_effects=True, vmem_limit_bytes=58 * 1024 * 1024),
    )(weights, dense.reshape((nz, ny) + dense.shape[1:]))


def body(occupied, virtual, cos_weights, pair_occ, pair_virt, partial_target_tile):
    owners = lax.axis_size("tile")
    groups = lax.axis_size("tau")
    size = occupied.shape[2]
    ny = 1
    while 2 * ny * 2 * ny <= owners:
        ny *= 2
    nz = owners // ny
    tile_bytes = 4 * size * size
    span = CHI_DEV
    while span > UNIT and span * tile_bytes * (
        nz * (1 + line_slots(ny)) + line_slots(nz) + 2
    ) > BUDGET:
        span //= 2
    results = []
    for q in range(CHI_DEV // span):
        dense = products(
            occupied[0], virtual[0], pair_occ, pair_virt, partial_target_tile,
            q * span, span, min(UNIT, span), owners, groups,
        )
        results.append(scatter(dense, cos_weights, ny, nz, groups))
    return results[0] if len(results) == 1 else jnp.concatenate(results, axis=1)


def solution(mesh):
    in_specs = (
        P("tau", "tile", None, None),
        P("tau", "tile", None, None),
        P(),
        P("tile", None),
        P("tile", None),
        P("tile"),
    )
    out_specs = P(None, "tile", "tau", None)
    return jax.shard_map(body, mesh=mesh, in_specs=in_specs, out_specs=out_specs, check_vma=False)
```

```python
import functools
import math

import jax
import jax.numpy as jnp
from jax import lax
from jax.experimental import pallas as pl
from jax.experimental.pallas import tpu as pltpu
from jax.sharding import PartitionSpec as P

CHI_DEV = 32
UNIT = 2
Z_FIRST = 3 / 16
BUDGET = 46 * 1024 * 1024
MESH = pl.DeviceIdType.MESH


def products_kernel(first, terms, chi_dev, occ_idx, virt_idx, target, occ, virt, out):
    owners, units, groups, each, rows, width = out.shape
    span = units * each
    count = target.shape[0]

    @pl.loop(0, owners)
    def _(d):
        out[d] = jnp.zeros(out.shape[1:], out.dtype)

    unroll = math.gcd(count, 4) if span == chi_dev else 1

    @pl.loop(0, count, unroll=unroll)
    def _(p):
        tile = target[p]
        owner = tile // chi_dev
        place = tile - owner * chi_dev - first

        def add():
            unit = place // each
            left = [occ[occ_idx[j, p]] for j in range(terms)]
            right = [virt[virt_idx[j, p]] for j in range(terms)]
            acc = jnp.dot(
                jnp.concatenate(left, axis=1),
                jnp.concatenate(right, axis=0),
                preferred_element_type=jnp.float32,
            )
            for g in range(groups):
                out[owner, unit, g, place - unit * each] += acc[g * rows : (g + 1) * rows]

        if span == chi_dev:
            add()
        else:
            pl.when((place >= 0) & (place < span))(add)


def products(occ, virt, occ_idx, virt_idx, target, first, span, each, owners, groups):
    terms = occ_idx.shape[1]
    size = occ.shape[1]
    smem = pl.BlockSpec(memory_space=pltpu.SMEM)
    vmem = pl.BlockSpec(memory_space=pltpu.VMEM)
    return pl.pallas_call(
        functools.partial(products_kernel, first, terms, CHI_DEV),
        out_shape=jax.ShapeDtypeStruct(
            (owners, span // each, groups, each, size // groups, size), jnp.float32
        ),
        in_specs=[smem, smem, smem, vmem, vmem],
        out_specs=vmem,
        compiler_params=pltpu.CompilerParams(vmem_limit_bytes=56 * 1024 * 1024),
        cost_estimate=pl.CostEstimate(
            flops=2 * target.shape[0] * terms * size**3 * span // CHI_DEV,
            bytes_accessed=occ.size * 4 + owners * span * size * size * 4,
            transcendentals=0,
        ),
    )(occ_idx.T, virt_idx.T, target, occ, virt)


def line_slots(n):
    if n == 1:
        return 0
    return 1 if n == 2 else 2 * (n - 1)


class Line:
    def __init__(self, n, place, device, own, slots, send_sem, recv_sem, hold=None):
        self.hold = hold
        self.n, self.place, self.device = n, place, device
        self.own, self.slots, self.send_sem, self.recv_sem = own, slots, send_sem, recv_sem

    def slot(self, right, d):
        if right:
            return d - 1
        return d if self.n == 2 else self.n - 1 + d

    def copy(self, right, u, d, src, back=False):
        s = self.slot(right, d)
        k = u * line_slots(self.n) + s
        return pltpu.make_async_remote_copy(
            src_ref=src,
            dst_ref=self.slots.at[s, u],
            send_sem=self.send_sem.at[k],
            recv_sem=self.recv_sem.at[k],
            device_id={"tile": self.device(1 if right != back else -1)},
            device_id_type=MESH,
        )

    def routes(self):
        for right in (True, False):
            for d in range(self.n - 1, 0, -1) if right else range(self.n - 1):
                yield right, d

    def launch(self, u):
        for right, d in self.routes():
            @pl.when(self.place == (0 if right else self.n - 1))
            def _():
                self.copy(right, u, d, self.own(d, u)).start()

    def merge(self, u):
        if self.n == 2:
            return
        for right, d in self.routes():
            inner = (self.place > 0) & (self.place < d) if right else (
                (self.place < self.n - 1) & (self.place > d))

            @pl.when(inner)
            def _():
                here = self.slots.at[self.slot(right, d), u]
                copy = self.copy(right, u, d, here)
                copy.wait_recv()
                own = self.own(d, u)
                if self.hold is not None:
                    buffer, sem = self.hold
                    fetch = pltpu.make_async_copy(own, buffer, sem)
                    fetch.start()
                    fetch.wait()
                    own = buffer
                here[...] += own[...]
                copy.start()

    def final(self, u, into):
        for right in (True, False):
            @pl.when(self.place > 0 if right else self.place < self.n - 1)
            def _():
                k = self.slot(right, self.place)
                here = self.slots.at[k, u]
                self.copy(right, u, self.place, here, back=True).wait_recv()
                into[...] += here[...]

    def drain(self, u):
        for right, d in self.routes():
            @pl.when(self.place < d if right else self.place > d)
            def _():
                self.copy(right, u, d, self.slots.at[self.slot(right, d), u]).wait_send()


def scatter_kernel(ny, nz, groups, weights, dense, out, mine, y_slots, z_slots, times,
                   load_sem, y_send, y_recv, z_send, z_recv, t_send, t_recv, hold, hold_sem,
                   both, z2_slots, y2_slots, both_sem, z2_send, z2_recv, y2_send, y2_recv):
    tau = lax.axis_index("tau")
    tile = lax.axis_index("tile")
    z, y = tile // ny, tile % ny
    units = mine.shape[0]
    lead = both.shape[0]
    last = units - lead
    each = mine.shape[3]
    freqs = out.shape[0]

    y_line = Line(ny, y, lambda step: tile + step, lambda d, u: dense.at[:, d, u],
                  y_slots, y_send, y_recv, (hold, hold_sem))
    z_line = Line(nz, z, lambda step: tile + step * ny, lambda d, u: mine.at[u, d],
                  z_slots, z_send, z_recv)

    z2_line = Line(nz, z, z_line.device, lambda d, u: both.at[u, d], z2_slots, z2_send, z2_recv)
    y2_line = Line(ny, y, y_line.device, lambda d, u: both.at[u, z, d], y2_slots, y2_send, y2_recv)

    barrier = pltpu.get_barrier_semaphore()
    for step in range(1, groups):
        pl.semaphore_signal(barrier, inc=1, device_id={"tau": (tau + step) % groups},
                            device_id_type=MESH)
    for step in range(1, ny):
        pl.semaphore_signal(barrier, inc=1, device_id={"tile": z * ny + (y + step) % ny},
                            device_id_type=MESH)
    for step in range(1, nz):
        pl.semaphore_signal(barrier, inc=1, device_id={"tile": (z + step) % nz * ny + y},
                            device_id_type=MESH)
    pl.semaphore_wait(barrier, groups - 1 + ny - 1 + nz - 1)

    def load(u):
        return pltpu.make_async_copy(dense.at[:, y, u], mine.at[u], load_sem.at[u])

    def swap(u, step):
        other = (tau + step) % groups
        return pltpu.make_async_remote_copy(
            src_ref=mine.at[u, z, other],
            dst_ref=times.at[u, tau],
            send_sem=t_send.at[u * groups + step],
            recv_sem=t_recv.at[u * groups + tau],
            device_id={"tau": other},
            device_id_type=MESH,
        )

    def arrived(u, source):
        return pltpu.make_async_remote_copy(
            src_ref=mine.at[u, z, 0],
            dst_ref=times.at[u, source],
            send_sem=t_send.at[u * groups],
            recv_sem=t_recv.at[u * groups + source],
            device_id={"tau": source},
            device_id_type=MESH,
        )

    def whole(w):
        return pltpu.make_async_copy(dense.at[:, :, last + w], both.at[w], both_sem.at[w])

    @pl.loop(0, lead)
    def _(w):
        whole(w).start()

    @pl.loop(0, last)
    def _(u):
        y_line.launch(u)
        load(u).start()

    @pl.loop(0, lead)
    def _(w):
        whole(w).wait()
        z2_line.launch(w)

    @pl.loop(0, lead)
    def _(w):
        z2_line.merge(w)

    @pl.loop(0, units + 2)
    def _(t):
        @pl.when(t < last)
        def _():
            load(t).wait()
            y_line.merge(t)
            y_line.final(t, mine.at[t])
            z_line.launch(t)

        @pl.when(t < lead)
        def _():
            z2_line.final(t, both.at[t, z])
            y2_line.launch(t)

        @pl.when((t >= 1) & (t < last + 1))
        def _():
            u = t - 1
            z_line.merge(u)
            z_line.final(u, mine.at[u, z])

        @pl.when((t >= last + 1) & (t < units + 1))
        def _():
            w = t - 1 - last
            y2_line.merge(w)
            mine[t - 1, z] = both[w, z, y]
            y2_line.final(w, mine.at[t - 1, z])

        @pl.when((t >= 1) & (t < units + 1))
        def _():
            u = t - 1
            for step in range(1, groups):
                swap(u, step).start()
            times[u, tau] = mine[u, z, tau]

        @pl.when(t >= 2)
        def _():
            u = t - 2
            for step in range(1, groups):
                arrived(u, (tau + step) % groups).wait_recv()
            for e in range(each):
                for k in range(freqs):
                    total = weights[k, 0] * times[u, 0, e]
                    for s in range(1, groups):
                        total += weights[k, s] * times[u, s, e]
                    out[k, u * each + e] = total

    @pl.loop(0, lead)
    def _(w):
        z2_line.drain(w)
        y2_line.drain(w)

    @pl.loop(0, last)
    def _(u):
        y_line.drain(u)
        z_line.drain(u)

    @pl.loop(0, units)
    def _(u):
        for step in range(1, groups):
            swap(u, step).wait_send()


def scatter(dense, weights, ny, nz, groups):
    owners, units, _, each, rows, width = dense.shape
    freqs = weights.shape[0]
    block = (groups, each, rows, width)
    lead = max(1, int(units * Z_FIRST))
    ys, zs = max(line_slots(ny), 1), max(line_slots(nz), 1)
    dma = pltpu.SemaphoreType.DMA
    return pl.pallas_call(
        functools.partial(scatter_kernel, ny, nz, groups),
        out_shape=jax.ShapeDtypeStruct((freqs, units * each, rows, width), jnp.float32),
        in_specs=[pl.BlockSpec(memory_space=pltpu.SMEM), pl.BlockSpec(memory_space=pl.ANY)],
        out_specs=pl.BlockSpec(memory_space=pltpu.VMEM),
        scratch_shapes=[
            pltpu.VMEM((units, nz) + block, jnp.float32),
            pltpu.VMEM((ys, units, nz) + block, jnp.float32),
            pltpu.VMEM((zs, units) + block, jnp.float32),
            pltpu.VMEM((units, groups, each, rows, width), jnp.float32),
            dma((units,)),
            dma((units * ys,)),
            dma((units * ys,)),
            dma((units * zs,)),
            dma((units * zs,)),
            dma((units * groups,)),
            dma((units * groups,)),
            pltpu.VMEM((nz,) + block if ny > 2 else (8, 128), jnp.float32),
            dma,
            pltpu.VMEM((lead, nz, ny) + block, jnp.float32),
            pltpu.VMEM((zs, lead, ny) + block, jnp.float32),
            pltpu.VMEM((ys, lead) + block, jnp.float32),
            dma((lead,)),
            dma((lead * zs,)),
            dma((lead * zs,)),
            dma((lead * ys,)),
            dma((lead * ys,)),
        ],
        compiler_params=pltpu.CompilerParams(
            collective_id=0, has_side_effects=True, vmem_limit_bytes=58 * 1024 * 1024),
    )(weights, dense.reshape((nz, ny) + dense.shape[1:]))


def body(occupied, virtual, cos_weights, pair_occ, pair_virt, partial_target_tile):
    owners = lax.axis_size("tile")
    groups = lax.axis_size("tau")
    size = occupied.shape[2]
    ny = 1
    while 2 * ny * 2 * ny <= owners:
        ny *= 2
    nz = owners // ny
    tile_bytes = 4 * size * size
    span = CHI_DEV
    while span > UNIT and span * tile_bytes * (
        nz * (1 + line_slots(ny)) + line_slots(nz) + 2
    ) > BUDGET:
        span //= 2
    results = []
    for q in range(CHI_DEV // span):
        dense = products(
            occupied[0], virtual[0], pair_occ, pair_virt, partial_target_tile,
            q * span, span, min(UNIT, span), owners, groups,
        )
        results.append(scatter(dense, cos_weights, ny, nz, groups))
    return results[0] if len(results) == 1 else jnp.concatenate(results, axis=1)


def solution(mesh):
    in_specs = (
        P("tau", "tile", None, None),
        P("tau", "tile", None, None),
        P(),
        P("tile", None),
        P("tile", None),
        P("tile"),
    )
    out_specs = P(None, "tile", "tau", None)
    return jax.shard_map(body, mesh=mesh, in_specs=in_specs, out_specs=out_specs, check_vma=False)
```

```python
import functools
import math

import jax
import jax.numpy as jnp
from jax import lax
from jax.experimental import pallas as pl
from jax.experimental.pallas import tpu as pltpu
from jax.sharding import PartitionSpec as P

CHI_DEV = 32
UNIT = 2
WINDOW = 3
Z_FIRST = 3 / 16
BUDGET = 46 * 1024 * 1024
MESH = pl.DeviceIdType.MESH


def products_kernel(first, terms, chi_dev, occ_idx, virt_idx, target, occ, virt, out):
    owners, units, groups, each, rows, width = out.shape
    span = units * each
    count = target.shape[0]

    @pl.loop(0, owners)
    def _(d):
        out[d] = jnp.zeros(out.shape[1:], out.dtype)

    unroll = math.gcd(count, 4) if span == chi_dev else 1

    @pl.loop(0, count, unroll=unroll)
    def _(p):
        tile = target[p]
        owner = tile // chi_dev
        place = tile - owner * chi_dev - first

        def add():
            unit = place // each
            left = [occ[occ_idx[j, p]] for j in range(terms)]
            right = [virt[virt_idx[j, p]] for j in range(terms)]
            acc = jnp.dot(
                jnp.concatenate(left, axis=1),
                jnp.concatenate(right, axis=0),
                preferred_element_type=jnp.float32,
            )
            for g in range(groups):
                out[owner, unit, g, place - unit * each] += acc[g * rows : (g + 1) * rows]

        if span == chi_dev:
            add()
        else:
            pl.when((place >= 0) & (place < span))(add)


def products(occ, virt, occ_idx, virt_idx, target, first, span, each, owners, groups):
    terms = occ_idx.shape[1]
    size = occ.shape[1]
    smem = pl.BlockSpec(memory_space=pltpu.SMEM)
    vmem = pl.BlockSpec(memory_space=pltpu.VMEM)
    return pl.pallas_call(
        functools.partial(products_kernel, first, terms, CHI_DEV),
        out_shape=jax.ShapeDtypeStruct(
            (owners, span // each, groups, each, size // groups, size), jnp.float32
        ),
        in_specs=[smem, smem, smem, vmem, vmem],
        out_specs=vmem,
        compiler_params=pltpu.CompilerParams(vmem_limit_bytes=56 * 1024 * 1024),
        cost_estimate=pl.CostEstimate(
            flops=2 * target.shape[0] * terms * size**3 * span // CHI_DEV,
            bytes_accessed=occ.size * 4 + owners * span * size * size * 4,
            transcendentals=0,
        ),
    )(occ_idx.T, virt_idx.T, target, occ, virt)


def line_slots(n):
    if n == 1:
        return 0
    return 1 if n == 2 else 2 * (n - 1)


class Line:
    def __init__(self, n, place, device, own, slots, send_sem, recv_sem, hold=None):
        self.hold = hold
        self.n, self.place, self.device = n, place, device
        self.own, self.slots, self.send_sem, self.recv_sem = own, slots, send_sem, recv_sem

    def slot(self, right, d):
        if right:
            return d - 1
        return d if self.n == 2 else self.n - 1 + d

    def copy(self, right, u, d, src, back=False):
        s = self.slot(right, d)
        k = u * line_slots(self.n) + s
        return pltpu.make_async_remote_copy(
            src_ref=src,
            dst_ref=self.slots.at[s, u],
            send_sem=self.send_sem.at[k],
            recv_sem=self.recv_sem.at[k],
            device_id={"tile": self.device(1 if right != back else -1)},
            device_id_type=MESH,
        )

    def routes(self):
        for right in (True, False):
            for d in range(self.n - 1, 0, -1) if right else range(self.n - 1):
                yield right, d

    def launch(self, u):
        for right, d in self.routes():
            @pl.when(self.place == (0 if right else self.n - 1))
            def _():
                self.copy(right, u, d, self.own(d, u)).start()

    def merge(self, u):
        if self.n == 2:
            return
        for right, d in self.routes():
            inner = (self.place > 0) & (self.place < d) if right else (
                (self.place < self.n - 1) & (self.place > d))

            @pl.when(inner)
            def _():
                here = self.slots.at[self.slot(right, d), u]
                copy = self.copy(right, u, d, here)
                copy.wait_recv()
                own = self.own(d, u)
                if self.hold is not None:
                    buffer, sem = self.hold
                    fetch = pltpu.make_async_copy(own, buffer, sem)
                    fetch.start()
                    fetch.wait()
                    own = buffer
                here[...] += own[...]
                copy.start()

    def final(self, u, into):
        for right in (True, False):
            @pl.when(self.place > 0 if right else self.place < self.n - 1)
            def _():
                k = self.slot(right, self.place)
                here = self.slots.at[k, u]
                self.copy(right, u, self.place, here, back=True).wait_recv()
                into[...] += here[...]

    def drain(self, u):
        for right, d in self.routes():
            @pl.when(self.place < d if right else self.place > d)
            def _():
                self.copy(right, u, d, self.slots.at[self.slot(right, d), u]).wait_send()


def scatter_kernel(ny, nz, groups, weights, dense, out, mine, y_slots, z_slots, times,
                   load_sem, y_send, y_recv, z_send, z_recv, t_send, t_recv, hold, hold_sem,
                   both, z2_slots, y2_slots, both_sem, z2_send, z2_recv, y2_send, y2_recv):
    tau = lax.axis_index("tau")
    tile = lax.axis_index("tile")
    z, y = tile // ny, tile % ny
    units = mine.shape[0]
    lead = both.shape[0]
    last = units - lead
    each = mine.shape[3]
    freqs = out.shape[0]

    y_line = Line(ny, y, lambda step: tile + step, lambda d, u: dense.at[:, d, u],
                  y_slots, y_send, y_recv, (hold, hold_sem))
    z_line = Line(nz, z, lambda step: tile + step * ny, lambda d, u: mine.at[u, d],
                  z_slots, z_send, z_recv)

    z2_line = Line(nz, z, z_line.device, lambda d, u: both.at[u, d], z2_slots, z2_send, z2_recv)
    y2_line = Line(ny, y, y_line.device, lambda d, u: both.at[u, z, d], y2_slots, y2_send, y2_recv)

    barrier = pltpu.get_barrier_semaphore()
    for step in range(1, groups):
        pl.semaphore_signal(barrier, inc=1, device_id={"tau": (tau + step) % groups},
                            device_id_type=MESH)
    for step in range(1, ny):
        pl.semaphore_signal(barrier, inc=1, device_id={"tile": z * ny + (y + step) % ny},
                            device_id_type=MESH)
    for step in range(1, nz):
        pl.semaphore_signal(barrier, inc=1, device_id={"tile": (z + step) % nz * ny + y},
                            device_id_type=MESH)
    pl.semaphore_wait(barrier, groups - 1 + ny - 1 + nz - 1)

    def load(u):
        return pltpu.make_async_copy(dense.at[:, y, u], mine.at[u], load_sem.at[u])

    def swap(u, step):
        other = (tau + step) % groups
        return pltpu.make_async_remote_copy(
            src_ref=mine.at[u, z, other],
            dst_ref=times.at[u, tau],
            send_sem=t_send.at[u * groups + step],
            recv_sem=t_recv.at[u * groups + tau],
            device_id={"tau": other},
            device_id_type=MESH,
        )

    def arrived(u, source):
        return pltpu.make_async_remote_copy(
            src_ref=mine.at[u, z, 0],
            dst_ref=times.at[u, source],
            send_sem=t_send.at[u * groups],
            recv_sem=t_recv.at[u * groups + source],
            device_id={"tau": source},
            device_id_type=MESH,
        )

    def whole(w):
        return pltpu.make_async_copy(dense.at[:, :, last + w], both.at[w], both_sem.at[w])

    @pl.loop(0, lead)
    def _(w):
        whole(w).start()

    @pl.loop(0, last)
    def _(u):
        @pl.when(u < WINDOW)
        def _():
            y_line.launch(u)

        load(u).start()

    @pl.loop(0, lead)
    def _(w):
        whole(w).wait()
        z2_line.launch(w)

    @pl.loop(0, lead)
    def _(w):
        z2_line.merge(w)

    @pl.loop(0, units + 2)
    def _(t):
        @pl.when(t < last)
        def _():
            load(t).wait()
            y_line.merge(t)
            y_line.final(t, mine.at[t])

            @pl.when(t + WINDOW < last)
            def _():
                y_line.launch(t + WINDOW)

            z_line.launch(t)

        @pl.when(t < lead)
        def _():
            z2_line.final(t, both.at[t, z])
            y2_line.launch(t)

        @pl.when((t >= 1) & (t < last + 1))
        def _():
            u = t - 1
            z_line.merge(u)
            z_line.final(u, mine.at[u, z])

        @pl.when((t >= last + 1) & (t < units + 1))
        def _():
            w = t - 1 - last
            y2_line.merge(w)
            mine[t - 1, z] = both[w, z, y]
            y2_line.final(w, mine.at[t - 1, z])

        @pl.when((t >= 1) & (t < units + 1))
        def _():
            u = t - 1
            for step in range(1, groups):
                swap(u, step).start()
            times[u, tau] = mine[u, z, tau]

        @pl.when(t >= 2)
        def _():
            u = t - 2
            for step in range(1, groups):
                arrived(u, (tau + step) % groups).wait_recv()
            for e in range(each):
                for k in range(freqs):
                    total = weights[k, 0] * times[u, 0, e]
                    for s in range(1, groups):
                        total += weights[k, s] * times[u, s, e]
                    out[k, u * each + e] = total

    @pl.loop(0, lead)
    def _(w):
        z2_line.drain(w)
        y2_line.drain(w)

    @pl.loop(0, last)
    def _(u):
        y_line.drain(u)
        z_line.drain(u)

    @pl.loop(0, units)
    def _(u):
        for step in range(1, groups):
            swap(u, step).wait_send()


def scatter(dense, weights, ny, nz, groups):
    owners, units, _, each, rows, width = dense.shape
    freqs = weights.shape[0]
    block = (groups, each, rows, width)
    lead = max(1, int(units * Z_FIRST))
    ys, zs = max(line_slots(ny), 1), max(line_slots(nz), 1)
    dma = pltpu.SemaphoreType.DMA
    return pl.pallas_call(
        functools.partial(scatter_kernel, ny, nz, groups),
        out_shape=jax.ShapeDtypeStruct((freqs, units * each, rows, width), jnp.float32),
        in_specs=[pl.BlockSpec(memory_space=pltpu.SMEM), pl.BlockSpec(memory_space=pl.ANY)],
        out_specs=pl.BlockSpec(memory_space=pltpu.VMEM),
        scratch_shapes=[
            pltpu.VMEM((units, nz) + block, jnp.float32),
            pltpu.VMEM((ys, units, nz) + block, jnp.float32),
            pltpu.VMEM((zs, units) + block, jnp.float32),
            pltpu.VMEM((units, groups, each, rows, width), jnp.float32),
            dma((units,)),
            dma((units * ys,)),
            dma((units * ys,)),
            dma((units * zs,)),
            dma((units * zs,)),
            dma((units * groups,)),
            dma((units * groups,)),
            pltpu.VMEM((nz,) + block if ny > 2 else (8, 128), jnp.float32),
            dma,
            pltpu.VMEM((lead, nz, ny) + block, jnp.float32),
            pltpu.VMEM((zs, lead, ny) + block, jnp.float32),
            pltpu.VMEM((ys, lead) + block, jnp.float32),
            dma((lead,)),
            dma((lead * zs,)),
            dma((lead * zs,)),
            dma((lead * ys,)),
            dma((lead * ys,)),
        ],
        compiler_params=pltpu.CompilerParams(
            collective_id=0, has_side_effects=True, vmem_limit_bytes=58 * 1024 * 1024),
    )(weights, dense.reshape((nz, ny) + dense.shape[1:]))


def body(occupied, virtual, cos_weights, pair_occ, pair_virt, partial_target_tile):
    owners = lax.axis_size("tile")
    groups = lax.axis_size("tau")
    size = occupied.shape[2]
    ny = 1
    while 2 * ny * 2 * ny <= owners:
        ny *= 2
    nz = owners // ny
    tile_bytes = 4 * size * size
    span = CHI_DEV
    while span > UNIT and span * tile_bytes * (
        nz * (1 + line_slots(ny)) + line_slots(nz) + 2
    ) > BUDGET:
        span //= 2
    results = []
    for q in range(CHI_DEV // span):
        dense = products(
            occupied[0], virtual[0], pair_occ, pair_virt, partial_target_tile,
            q * span, span, min(UNIT, span), owners, groups,
        )
        results.append(scatter(dense, cos_weights, ny, nz, groups))
    return results[0] if len(results) == 1 else jnp.concatenate(results, axis=1)


def solution(mesh):
    in_specs = (
        P("tau", "tile", None, None),
        P("tau", "tile", None, None),
        P(),
        P("tile", None),
        P("tile", None),
        P("tile"),
    )
    out_specs = P(None, "tile", "tau", None)
    return jax.shard_map(body, mesh=mesh, in_specs=in_specs, out_specs=out_specs, check_vma=False)
```
